256 devices in a mesh: row: 8 (over z_hi, x), col: 32 (over z_lo, y, core).
Axes of the slice: x: 4, y: 4, z: 8 (z_hi: 2, z_lo: 4; z = z_hi * 4 + z_lo), core: 2. Of those that a mesh axis runs over, the one named last changes fastest.
Arguments:
- matrix: bfloat16 [3072, 262144], P('row', 'col'), may hold values from -0.01171875 to 0.01171875
- probes: bfloat16 [262144, 128], P('col'), may hold values from -6 to 6
Outputs:
- krylov: bfloat16 [2, 262144, 128], P(None, 'col')
The draws below stay inside these ranges and needn't reach their ends.
All inputs are finite; a program needn't handle non-finite values.
Results may differ from the reference program's by a relative error of at most 0.0054.
Values may be sent and summed in bfloat16 or wider, within the bound.
A program may use at most 64 MiB of HBM per device.

```python
import math
import jax
import jax.numpy as jnp
from jax import lax

N = 262144
K = 128
ITERS = 2
M = 3072


def level_of(own_key, extent, split, smallest, largest):
    gain, own = 1.0, jax.random.fold_in(own_key, 6)
    for axis_at, shards_of in split:
        draws = jnp.exp(jax.random.uniform(jax.random.fold_in(own, axis_at), (shards_of,), jnp.float32, smallest / len(split), largest / len(split)))
        gain = gain * jnp.repeat(draws, extent[axis_at] // shards_of).reshape([-1 if axis == axis_at else 1 for axis in range(len(extent))])
    return gain


def bell_draw(own_key, extent, scale, limit, pieces=(), kind=jnp.bfloat16):
    result = jax.random.normal(own_key, extent, jnp.float32) * scale
    if len(pieces) > 0:
        result = level_of(own_key, extent, pieces, -0.22, 0.18) * result
    return jnp.clip(result, min=-limit, max=limit).astype(kind)


def setup_inputs(seed: int = 0) -> dict:
    streams_of = jax.random.split(jax.random.key(seed), 3)
    return {
        "matrix": bell_draw(streams_of[0], (M, N), N ** -0.5, 0.01171875, ((0, 8), (1, 32))),
        "probes": bell_draw(streams_of[1], (N, K), 1.0, 6.0, ((0, 32),)),
    }


def reference(matrix, probes):
    stretch = math.sqrt(N / M)
    current = probes
    results = []
    for level in range(ITERS):
        factor = 1.0 if level == 0 else 1.0 / stretch
        partial_value = jnp.dot(matrix, current, preferred_element_type=jnp.float32)
        reduced = (partial_value * factor).astype(jnp.bfloat16)
        back = lax.dot_general(matrix, reduced, (((0,), (0,)), ((), ())), preferred_element_type=jnp.float32)
        current = (back * stretch).astype(jnp.bfloat16)
        results.append(current)
    return jnp.stack(results)
```

```python
import functools
import math

import jax
import jax.numpy as jnp
from jax import lax
from jax.experimental import pallas as pl
from jax.experimental.pallas import tpu as pltpu
from jax.sharding import Mesh
from jax.sharding import PartitionSpec as P

AXES = ("zh", "x", "zl", "y", "core")
SIZES = (2, 4, 4, 4, 2)
NX, NZL, NY, NC = 4, 4, 4, 2
ITERS = 2
STREAMS = 4
LOADS = 8
F32, BF16 = jnp.float32, jnp.bfloat16
MESH_ID = pl.DeviceIdType.MESH


def kernel(
    stretch,
    a_hbm, p_hbm, out,
    a, p, z1, zsend, zr1, zs2, zr2, zg, ysend, yown, yr, hs, hr,
    load_sem, send_sem, recv_sem,
):
    rows, width = a.shape
    group = width // NX
    depth = out.shape[2] // STREAMS
    part = depth // NY
    step = width // LOADS
    x, zl, y, core = (lax.axis_index(n) for n in ("x", "zl", "y", "core"))
    zh = lax.axis_index("zh")
    me = y * NC + core

    def columns(b):
        return pl.ds(b * step, step)

    loads = []
    for b in range(LOADS):
        pair = (
            pltpu.make_async_copy(a_hbm.at[:, columns(b)], a.at[:, columns(b)], load_sem.at[0, b]),
            pltpu.make_async_copy(p_hbm.at[columns(b)], p.at[columns(b)], load_sem.at[1, b]),
        )
        for copy in pair:
            copy.start()
        loads.append(pair)

    near = [(dy, dc) for dy in range(NY) for dc in range(NC) if dy or dc]

    def near_id(dy, dc):
        return {"y": lax.rem(y + dy, NY), "core": lax.rem(core + dc, NC)}

    def x_id(dx):
        return {"x": lax.rem(x + dx, NX)}

    def zl_id(dz):
        return {"zl": lax.rem(zl + dz, NZL)}

    def y_id(dy):
        return {"y": lax.rem(y + dy, NY)}

    half_id = {"zh": 1 - zh}
    x_order = (2, 1, 3)

    barrier = pltpu.get_barrier_semaphore()
    peers = [near_id(*d) for d in near] + [zl_id(d) for d in (1, 2, 3)]
    peers += [x_id(d) for d in (1, 2, 3)] + [half_id]
    for peer in peers:
        pl.semaphore_signal(barrier, inc=1, device_id=peer, device_id_type=MESH_ID)

    def send(src, dst, j, stage, peer):
        pltpu.make_async_remote_copy(
            src_ref=src, dst_ref=dst, send_sem=send_sem.at[j, stage], recv_sem=recv_sem.at[j, stage],
            device_id=peer, device_id_type=MESH_ID,
        ).start()

    def done(ref, j, stage):
        return pltpu.make_async_remote_copy(
            src_ref=ref, dst_ref=ref, send_sem=send_sem.at[j, stage], recv_sem=recv_sem.at[j, stage],
            device_id=half_id, device_id_type=MESH_ID,
        )

    def stream_rows(s):
        return pl.ds(s * depth, depth)

    def z_send(j, value):
        zsend[j] = value.reshape(NY, part, rows)
        zr1[j, me] = zsend[j, y]
        for dy, dc in near:
            peer = near_id(dy, dc)
            send(zsend.at[j, peer["y"]], zr1.at[j, me], j, 0, peer)

    def t1(s):
        j = STREAMS + s
        done(out.at[0, pl.ds(0, NX - 1), stream_rows(s)], s, 5).wait_recv()
        total = jnp.zeros((depth, rows), F32)
        for b in range(NX):
            total += lax.dot_general(
                out[0, b, stream_rows(s), :], a[:, pl.ds(b * group, group)],
                (((1,), (1,)), ((), ())), preferred_element_type=F32,
            )
        z_send(j, total)

    def t2(j):
        done(zr1.at[j, pl.ds(0, NY * NC - 1)], j, 0).wait_recv()
        total = zr1[j, 0]
        for i in range(1, NY * NC):
            total += zr1[j, i]
        zs2[j] = total
        zr2[j, zl] = total
        for dz in (1, 2, 3):
            send(zs2.at[j], zr2.at[j, zl], j, 1, zl_id(dz))

    def t3(j, factor):
        done(zr2.at[j, pl.ds(0, NZL - 1)], j, 1).wait_recv()
        total = zr2[j, 0]
        for i in range(1, NZL):
            total += zr2[j, i]
        zg[j, y] = (total * factor).astype(BF16).astype(F32)
        for dy in (1, 2, 3):
            send(zg.at[j, y], zg.at[j, y], j, 2, y_id(dy))

    def t4(j):
        done(zg.at[j, pl.ds(0, NY - 1)], j, 2).wait_recv()
        z = zg[j].reshape(depth, rows).astype(BF16)

        def block(owner):
            return jnp.dot(
                z, a[:, pl.ds(pl.multiple_of(owner * group, group), group)],
                preferred_element_type=F32,
            )

        for i, dx in enumerate(x_order):
            ysend[j, i] = block(lax.rem(x + dx, NX)).astype(BF16)
            send(ysend.at[j, i], yr.at[j, i], j, 3, x_id(dx))
        yown[j] = block(x)

    def t5(j):
        done(yr.at[j], j, 3).wait_recv()
        total = yown[j]
        for i in range(NX - 1):
            total += yr[j, i].astype(F32)
        hs[j] = total.astype(BF16)
        send(hs.at[j], hr.at[j], j, 4, half_id)

    def t6(k, s):
        j = k * STREAMS + s
        done(hr.at[j], j, 4).wait_recv()
        total = (hs[j].astype(F32) + hr[j].astype(F32)) * stretch
        place = out.at[k, x, stream_rows(s)]
        out[k, x, stream_rows(s), :] = total.astype(BF16)
        for dx in x_order:
            send(place, place, j, 5, x_id(dx))

    for b in range(LOADS):
        for copy in loads[b]:
            copy.wait()
        term = jnp.dot(a[:, columns(b)], p[columns(b), :], preferred_element_type=F32)
        if b == 0:
            z1[...] = term
        else:
            z1[...] += term
    first = z1[...].T
    pl.semaphore_wait(barrier, len(peers))

    S = STREAMS
    for s in range(S):
        z_send(s, first[s * depth : (s + 1) * depth])
    for s in range(S):
        t2(s)
    for s in range(S):
        t3(s, 1.0)
    for s in range(S):
        t4(s)
    inv = 1.0 / stretch
    plan = (
        50, 51, 60, 52, 61, 53, 62, 10, 63, 11, 24, 12, 34, 25, 44, 13, 35, 26,
        45, 27, 36, 54, 46, 37, 55, 47, 64, 56, 65, 57, 66, 67,
    )
    for task in plan:
        kind, j = divmod(task, 10)
        if kind == 1:
            t1(j)
        elif kind == 2:
            t2(j)
        elif kind == 3:
            t3(j, inv)
        elif kind == 4:
            t4(j)
        elif kind == 5:
            t5(j)
        else:
            t6(*divmod(j, S))
    for s in range(S):
        done(out.at[1, pl.ds(0, NX - 1), stream_rows(s)], S + s, 5).wait_recv()
    for j in range(ITERS * S):
        for stage, ref in enumerate(
            (
                zr1.at[j, pl.ds(0, NY * NC - 1)], zr2.at[j, pl.ds(0, NZL - 1)], zg.at[j, pl.ds(0, NY - 1)],
                ysend.at[j], hs.at[j], out.at[0, pl.ds(0, NX - 1), stream_rows(0)],
            )
        ):
            done(ref, j, stage).wait_send()


def body(matrix, probes):
    rows, width = matrix.shape
    probe = probes.shape[1]
    m_total = rows * SIZES[0] * SIZES[1]
    n_total = width * SIZES[2] * SIZES[3] * SIZES[4]
    group, depth = width // NX, probe // STREAMS
    part, count = depth // NY, ITERS * STREAMS
    blocks = pl.pallas_call(
        functools.partial(kernel, math.sqrt(n_total / m_total)),
        out_shape=jax.ShapeDtypeStruct((ITERS, NX, probe, group), BF16),
        in_specs=[pl.BlockSpec(memory_space=pl.ANY)] * 2,
        out_specs=pl.BlockSpec(memory_space=pltpu.VMEM),
        scratch_shapes=[
            pltpu.VMEM((rows, width), BF16),
            pltpu.VMEM((width, probe), BF16),
            pltpu.VMEM((rows, probe), F32),
            pltpu.VMEM((count, NY, part, rows), F32),
            pltpu.VMEM((count, NY * NC, part, rows), F32),
            pltpu.VMEM((count, part, rows), F32),
            pltpu.VMEM((count, NZL, part, rows), F32),
            pltpu.VMEM((count, NY, part, rows), F32),
            pltpu.VMEM((count, NX - 1, depth, group), BF16),
            pltpu.VMEM((count, depth, group), F32),
            pltpu.VMEM((count, NX - 1, depth, group), BF16),
            pltpu.VMEM((count, depth, group), BF16),
            pltpu.VMEM((count, depth, group), BF16),
            pltpu.SemaphoreType.DMA((2, LOADS)),
            pltpu.SemaphoreType.DMA((count, 6)),
            pltpu.SemaphoreType.DMA((count, 6)),
        ],
        compiler_params=pltpu.CompilerParams(
            collective_id=0, has_side_effects=True, vmem_limit_bytes=56 * 1024 * 1024
        ),
    )(matrix, probes)
    return jnp.swapaxes(blocks, 2, 3).reshape(ITERS, width, probe)


def solution(mesh):
    torus = Mesh(mesh.devices.reshape(SIZES), AXES)
    col = ("zl", "y", "core")
    return jax.shard_map(
        body, mesh=torus, in_specs=(P(("zh", "x"), col), P(col, None)),
        out_specs=P(None, col, None), check_vma=False,
    )
```

```python
import functools
import math

import jax
import jax.numpy as jnp
from jax import lax
from jax.experimental import pallas as pl
from jax.experimental.pallas import tpu as pltpu
from jax.sharding import Mesh
from jax.sharding import PartitionSpec as P

AXES = ("zh", "x", "zl", "y", "core")
SIZES = (2, 4, 4, 4, 2)
NX, NZL, NY, NC = 4, 4, 4, 2
ITERS = 2
STREAMS = 4
PARTS = 2
LOADS = 8
PLAN = (
    0, 1, 2, 3, 1000, 1001, 1002, 1003, 200, 201, 202, 203, 300, 301, 302, 303, 400, 900, 401, 402, 901, 403, 500,
    902, 501, 903, 502, 503, 504, 505, 506, 507, 600, 601, 602, 603, 604, 700, 605, 606, 607, 701, 800, 702, 801,
    703, 802, 104, 704, 803, 705, 804, 105, 204, 706, 805, 707, 806, 106, 304, 205, 807, 107, 305, 404, 206, 904,
    508, 405, 509, 306, 905, 207, 608, 510, 406, 906, 511, 609, 307, 610, 512, 513, 708, 407, 907, 611, 709, 612,
    613, 808, 710, 514, 515, 711, 809, 712, 810, 614, 615, 713, 811, 812, 813, 714, 715, 814, 815,
)
F32, BF16 = jnp.float32, jnp.bfloat16
MESH_ID = pl.DeviceIdType.MESH


def kernel(
    stretch,
    a_hbm, p_hbm, out,
    a, at, p, z1, zpart, zsend, zr1, zs2, zr2, zg, far, alone, held, yown, passed, yr, hs, hr,
    load_sem, z_send_sem, z_recv_sem, y_send_sem, y_recv_sem,
):
    rows, width = a.shape
    group = width // NX
    half = group // 2
    depth = out.shape[2] // STREAMS
    part = depth // NY
    sub = depth // PARTS
    step = width // LOADS
    x, zl, y, core = (lax.axis_index(n) for n in ("x", "zl", "y", "core"))
    zh = lax.axis_index("zh")
    me = y * NC + core

    def columns(b):
        return pl.ds(b * step, step)

    loads = []
    for b in range(LOADS):
        pair = (
            pltpu.make_async_copy(a_hbm.at[:, columns(b)], a.at[:, columns(b)], load_sem.at[0, b]),
            pltpu.make_async_copy(p_hbm.at[columns(b)], p.at[columns(b)], load_sem.at[1, b]),
        )
        for copy in pair:
            copy.start()
        loads.append(pair)

    near = [(dy, dc) for dy in range(NY) for dc in range(NC) if dy or dc]

    def near_id(dy, dc):
        return {"y": lax.rem(y + dy, NY), "core": lax.rem(core + dc, NC)}

    def x_id(dx):
        return {"x": lax.rem(x + dx, NX)}

    def zl_id(dz):
        return {"zl": lax.rem(zl + dz, NZL)}

    def y_id(dy):
        return {"y": lax.rem(y + dy, NY)}

    other = {"zh": 1 - zh}
    right, left = x_id(1), x_id(3)

    barrier = pltpu.get_barrier_semaphore()
    peers = [near_id(*d) for d in near] + [zl_id(d) for d in (1, 2, 3)]
    peers += [x_id(d) for d in (1, 2, 3)] + [other]
    for peer in peers:
        pl.semaphore_signal(barrier, inc=1, device_id=peer, device_id_type=MESH_ID)

    sent, got = {}, set()
    low, high = pl.ds(0, half), pl.ds(half, half)

    def sems(j, stage):
        if stage < 3:
            return {"send_sem": z_send_sem.at[j, stage], "recv_sem": z_recv_sem.at[j, stage]}
        return {"send_sem": y_send_sem.at[j, stage - 3], "recv_sem": y_recv_sem.at[j, stage - 3]}

    def send(src, dst, j, stage, peer):
        sent[j, stage] = 1
        pltpu.make_async_remote_copy(
            src_ref=src, dst_ref=dst, device_id=peer, device_id_type=MESH_ID, **sems(j, stage)
        ).start()

    def done(j, stage):
        r = pl.ds(0, sub)
        ref = (
            lambda: zr1.at[j, pl.ds(0, NY * NC - 1)], lambda: zr2.at[j, pl.ds(0, NZL - 1)],
            lambda: zg.at[j, pl.ds(0, NY - 1)], lambda: passed.at[j], lambda: yr.at[j], lambda: hr.at[j],
            lambda: out.at[0, pl.ds(0, 2), r], lambda: out.at[0, 0, r],
        )[stage]()
        return pltpu.make_async_remote_copy(
            src_ref=ref, dst_ref=ref, device_id=other, device_id_type=MESH_ID, **sems(j, stage)
        )

    def arrived(j, stage):
        got.add((j, stage))
        done(j, stage).wait_recv()

    def stream_rows(s):
        return pl.ds(s * depth, depth)

    def place_of(i):
        j, h = divmod(i, PARTS)
        k, s = divmod(j, STREAMS)
        return k, s, h == PARTS - 1, pl.ds(s * depth + h * sub, sub)

    def z_send(j, value):
        zsend[j] = value.reshape(NY, part, rows)
        zr1[j, me] = zsend[j, y]
        for dy, dc in near:
            peer = near_id(dy, dc)
            send(zsend.at[j, peer["y"]], zr1.at[j, me], j, 0, peer)

    def term(s, owner):
        return jnp.dot(
            out[0, owner, stream_rows(s), :], at[pl.ds(pl.multiple_of(owner * group, group), group), :],
            preferred_element_type=F32,
        )

    def t1(j):
        s = j - STREAMS

        for h in range(PARTS):
            arrived(s * PARTS + h, 7)
        z_send(j, zpart[s] + term(s, lax.rem(x + 2, NX)))

    def t2(j):
        arrived(j, 0)
        total = zr1[j, 0]
        for i in range(1, NY * NC):
            total += zr1[j, i]
        zs2[j] = total
        zr2[j, zl] = total
        for dz in (1, 2, 3):
            send(zs2.at[j], zr2.at[j, zl], j, 1, zl_id(dz))

    def t3(j):
        arrived(j, 1)
        total = zr2[j, 0]
        for i in range(1, NZL):
            total += zr2[j, i]
        factor = 1.0 if j < STREAMS else 1.0 / stretch
        zg[j, y] = (total * factor).astype(BF16).astype(F32)
        for dy in (1, 2, 3):
            send(zg.at[j, y], zg.at[j, y], j, 2, y_id(dy))

    def block(j, owner):
        z = zg[j].reshape(depth, rows).astype(BF16)
        return jnp.dot(
            z, a[:, pl.ds(pl.multiple_of(owner * group, group), group)],
            preferred_element_type=F32,
        )

    def pieces(j):
        return [(j * PARTS + h, slice(h * sub, (h + 1) * sub)) for h in range(PARTS)]

    def t4(j):
        arrived(j, 2)
        value = block(j, lax.rem(x + 2, NX)).astype(BF16)
        for i, r in pieces(j):
            far[i, 0] = value[r, :half]
            far[i, 1] = value[r, half:]
            send(far.at[i, 0], passed.at[i, 0], i, 3, right)
            send(far.at[i, 1], passed.at[i, 1], i, 3, left)

    def t9(j):
        value = block(j, right["x"])
        for i, r in pieces(j):
            held[i, 0] = value[r, :half]
            alone[i, 0] = value[r, half:].astype(BF16)
            send(alone.at[i, 0], yr.at[i, 0, 1], i, 4, right)
        value = block(j, left["x"])
        for i, r in pieces(j):
            held[i, 1] = value[r, half:]
            alone[i, 1] = value[r, :half].astype(BF16)
            send(alone.at[i, 1], yr.at[i, 1, 0], i, 4, left)
        value = block(j, x)
        for i, r in pieces(j):
            yown[i] = value[r]

    def t5(i):
        arrived(i, 3)
        for n, peer in enumerate((right, left)):
            far[i, 2 + n] = (held[i, n] + passed[i, n].astype(F32)).astype(BF16)
            send(far.at[i, 2 + n], yr.at[i, n, n], i, 4, peer)

    def t6(i):
        arrived(i, 4)
        for n, cols in enumerate((low, high)):
            total = yown[i, :, cols] + yr[i, 0, n].astype(F32) + yr[i, 1, n].astype(F32)
            hs[i, :, cols] = total.astype(BF16)
        send(hs.at[i], hr.at[i], i, 5, other)

    def t7(i):
        k, s, last, r = place_of(i)
        arrived(i, 5)
        total = (hs[i].astype(F32) + hr[i].astype(F32)) * stretch
        out[k, x, r, :] = total.astype(BF16)
        place = out.at[k, x, r]
        for peer in (right, left):
            send(place, place, i, 6, peer)
        if k == 0 and last:
            zpart[s] = term(s, x)

    def t8(i):
        k, s, last, r = place_of(i)
        arrived(i, 6)
        for source, cols, peer in ((left, low, right), (right, high, left)):
            place = out.at[k, source["x"], r, cols]
            send(place, place, i, 7, peer)
        if k == 0 and last:
            zpart[s] += term(s, right["x"]) + term(s, left["x"])

    for b in range(LOADS):
        for copy in loads[b]:
            copy.wait()
        product = jnp.dot(a[:, columns(b)], p[columns(b), :], preferred_element_type=F32)
        if b == 0:
            z1[...] = product
        else:
            z1[...] += product
    first = z1[...].T
    pl.semaphore_wait(barrier, len(peers))

    def t0(j):
        z_send(j, first[j * depth : (j + 1) * depth])

    def t10(q):
        cols = pl.ds(q * group, group)
        at[cols, :] = a[:, cols].T

    tasks = (t0, t1, t2, t3, t4, t5, t6, t7, t8, t9, t10)
    for task in PLAN:
        kind, j = divmod(task, 100)
        tasks[kind](j)
    for j, stage in sent:
        if (j, stage) not in got:
            arrived(j, stage)
    for j, stage in sent:
        done(j, stage).wait_send()


def turn(blocks, out, turned, sems):
    group = blocks.shape[3]
    copies = []
    for k in range(ITERS):
        for b in range(NX):
            rows = pl.ds(b * group, group)
            turned[k, rows, :] = blocks[k, b].T
            copy = pltpu.make_async_copy(turned.at[k, rows], out.at[k, rows], sems.at[k, b])
            copy.start()
            copies.append(copy)
    for copy in copies:
        copy.wait()


def body(matrix, probes):
    rows, width = matrix.shape
    probe = probes.shape[1]
    m_total = rows * SIZES[0] * SIZES[1]
    n_total = width * SIZES[2] * SIZES[3] * SIZES[4]
    group, depth = width // NX, probe // STREAMS
    part, half, count = depth // NY, group // 2, ITERS * STREAMS
    sub, pieces = depth // PARTS, ITERS * STREAMS * PARTS
    blocks = pl.pallas_call(
        functools.partial(kernel, math.sqrt(n_total / m_total)),
        out_shape=jax.ShapeDtypeStruct((ITERS, NX, probe, group), BF16),
        in_specs=[pl.BlockSpec(memory_space=pltpu.HBM)] * 2,
        out_specs=pl.BlockSpec(memory_space=pltpu.VMEM),
        scratch_shapes=[
            pltpu.VMEM((rows, width), BF16),
            pltpu.VMEM((width, rows), BF16),
            pltpu.VMEM((width, probe), BF16),
            pltpu.VMEM((rows, probe), F32),
            pltpu.VMEM((STREAMS, depth, rows), F32),
            pltpu.VMEM((count, NY, part, rows), F32),
            pltpu.VMEM((count, NY * NC, part, rows), F32),
            pltpu.VMEM((count, part, rows), F32),
            pltpu.VMEM((count, NZL, part, rows), F32),
            pltpu.VMEM((count, NY, part, rows), F32),
            pltpu.VMEM((pieces, 4, sub, half), BF16),
            pltpu.VMEM((pieces, 2, sub, half), BF16),
            pltpu.VMEM((pieces, 2, sub, half), F32),
            pltpu.VMEM((pieces, sub, group), F32),
            pltpu.VMEM((pieces, 2, sub, half), BF16),
            pltpu.VMEM((pieces, 2, 2, sub, half), BF16),
            pltpu.VMEM((pieces, sub, group), BF16),
            pltpu.VMEM((pieces, sub, group), BF16),
            pltpu.SemaphoreType.DMA((2, LOADS)),
            pltpu.SemaphoreType.DMA((count, 3)),
            pltpu.SemaphoreType.DMA((count, 3)),
            pltpu.SemaphoreType.DMA((pieces, 5)),
            pltpu.SemaphoreType.DMA((pieces, 5)),
        ],
        compiler_params=pltpu.CompilerParams(
            collective_id=0, has_side_effects=True, vmem_limit_bytes=44 * 1024 * 1024
        ),
    )(*(pltpu.with_memory_space_constraint(v, pltpu.HBM) for v in (matrix, probes)))
    return pl.pallas_call(
        turn,
        out_shape=jax.ShapeDtypeStruct((ITERS, width, probe), BF16),
        in_specs=[pl.BlockSpec(memory_space=pltpu.VMEM)],
        out_specs=pl.BlockSpec(memory_space=pl.ANY),
        scratch_shapes=[
            pltpu.VMEM((ITERS, width, probe), BF16),
            pltpu.SemaphoreType.DMA((ITERS, NX)),
        ],
        compiler_params=pltpu.CompilerParams(vmem_limit_bytes=24 * 1024 * 1024),
    )(blocks)


def solution(mesh):
    torus = Mesh(mesh.devices.reshape(SIZES), AXES)
    col = ("zl", "y", "core")
    return jax.shard_map(
        body, mesh=torus, in_specs=(P(("zh", "x"), col), P(col, None)),
        out_specs=P(None, col, None), check_vma=False,
    )
```

```python
import functools
import math

import jax
import jax.numpy as jnp
from jax import lax
from jax.experimental import pallas as pl
from jax.experimental.pallas import tpu as pltpu
from jax.sharding import Mesh
from jax.sharding import PartitionSpec as P

AXES = ("zh", "x", "zl", "y", "core")
SIZES = (2, 4, 4, 4, 2)
NX, NZL, NY, NC = 4, 4, 4, 2
ITERS = 2
STREAMS = 4
PARTS = 2
STRAIGHT_SUMS = (0, 1)
STRAIGHT_COPIES = (14, 15)
LOADS = 8
PLAN = (
    0, 1000, 1, 2, 3, 200, 201, 1003, 300, 203, 202, 400, 301, 1002, 303, 302, 900, 401, 403, 901, 600, 502, 903,
    503, 601, 1001, 402, 602, 506, 507, 700, 603, 902, 606, 504, 701, 607, 505, 800, 702, 703, 604, 801, 605, 706,
    803, 802, 104, 707, 704, 705, 105, 204, 806, 807, 804, 805, 205, 304, 107, 106, 305, 404, 207, 904, 206, 508,
    405, 307, 509, 905, 510, 306, 608, 511, 407, 609, 907, 406, 611, 514, 906, 708, 610, 512, 709, 513, 614, 515,
    808, 711, 612, 710, 809, 613, 615, 714, 712, 810, 811, 713, 812, 715, 813,
)
F32, BF16 = jnp.float32, jnp.bfloat16
MESH_ID = pl.DeviceIdType.MESH


def kernel(
    stretch,
    a_hbm, p_hbm, out,
    a, at, p, z1, zpart, zsend, zr1, zs2, zr2, zg, far, alone, held, yown, passed, yr, hs, hr,
    load_sem, z_send_sem, z_recv_sem, y_send_sem, y_recv_sem,
):
    rows, width = a.shape
    group = width // NX
    half = group // 2
    depth = out.shape[2] // STREAMS
    part = depth // NY
    sub = depth // PARTS
    step = width // LOADS
    x, zl, y, core = (lax.axis_index(n) for n in ("x", "zl", "y", "core"))
    zh = lax.axis_index("zh")
    me = y * NC + core

    def columns(b):
        return pl.ds(b * step, step)

    loads = []
    for b in range(LOADS):
        pair = (
            pltpu.make_async_copy(a_hbm.at[:, columns(b)], a.at[:, columns(b)], load_sem.at[0, b]),
            pltpu.make_async_copy(p_hbm.at[columns(b)], p.at[columns(b)], load_sem.at[1, b]),
        )
        for copy in pair:
            copy.start()
        loads.append(pair)

    near = [(dy, dc) for dy in range(NY) for dc in range(NC) if dy or dc]

    def near_id(dy, dc):
        return {"y": lax.rem(y + dy, NY), "core": lax.rem(core + dc, NC)}

    def x_id(dx):
        return {"x": lax.rem(x + dx, NX)}

    def zl_id(dz):
        return {"zl": lax.rem(zl + dz, NZL)}

    def y_id(dy):
        return {"y": lax.rem(y + dy, NY)}

    other = {"zh": 1 - zh}
    right, left, across = x_id(1), x_id(3), x_id(2)

    barrier = pltpu.get_barrier_semaphore()
    peers = [near_id(*d) for d in near] + [zl_id(d) for d in (1, 2, 3)]
    peers += [x_id(d) for d in (1, 2, 3)] + [other]
    for peer in peers:
        pl.semaphore_signal(barrier, inc=1, device_id=peer, device_id_type=MESH_ID)

    sent, got = {}, set()
    low, high = pl.ds(0, half), pl.ds(half, half)

    def sems(j, stage):
        if stage < 3:
            return {"send_sem": z_send_sem.at[j, stage], "recv_sem": z_recv_sem.at[j, stage]}
        return {"send_sem": y_send_sem.at[j, stage - 3], "recv_sem": y_recv_sem.at[j, stage - 3]}

    def send(src, dst, j, stage, peer):
        sent[j, stage] = 1
        pltpu.make_async_remote_copy(
            src_ref=src, dst_ref=dst, device_id=peer, device_id_type=MESH_ID, **sems(j, stage)
        ).start()

    def done(j, stage):
        r = pl.ds(0, sub)
        ref = (
            lambda: zr1.at[j, pl.ds(0, NY * NC - 1)], lambda: zr2.at[j, pl.ds(0, NZL - 1)],
            lambda: zg.at[j, pl.ds(0, NY - 1)], lambda: passed.at[j], lambda: yr.at[j], lambda: hr.at[j],
            lambda: out.at[0, pl.ds(0, 2), r], lambda: out.at[0, 0, r],
        )[stage]()
        return pltpu.make_async_remote_copy(
            src_ref=ref, dst_ref=ref, device_id=other, device_id_type=MESH_ID, **sems(j, stage)
        )

    def arrived(j, stage):
        got.add((j, stage))
        done(j, stage).wait_recv()

    def stream_rows(s):
        return pl.ds(s * depth, depth)

    def place_of(i):
        j, h = divmod(i, PARTS)
        k, s = divmod(j, STREAMS)
        return k, s, pl.ds(s * depth + h * sub, sub)

    counts = {}

    def whole(kind, s):
        counts[kind, s] = counts.get((kind, s), 0) + 1
        return counts[kind, s] == PARTS

    def z_send(j, value):
        zsend[j] = value.reshape(NY, part, rows)
        zr1[j, me] = zsend[j, y]
        for dy, dc in near:
            peer = near_id(dy, dc)
            send(zsend.at[j, peer["y"]], zr1.at[j, me], j, 0, peer)

    def term(s, owner):
        return jnp.dot(
            out[0, owner, stream_rows(s), :], at[pl.ds(pl.multiple_of(owner * group, group), group), :],
            preferred_element_type=F32,
        )

    def t1(j):
        s = j - STREAMS

        for h in range(PARTS):
            arrived(s * PARTS + h, 7)
        z_send(j, zpart[s] + term(s, across["x"]))

    def t2(j):
        arrived(j, 0)
        total = zr1[j, 0]
        for i in range(1, NY * NC):
            total += zr1[j, i]
        zs2[j] = total
        zr2[j, zl] = total
        for dz in (1, 2, 3):
            send(zs2.at[j], zr2.at[j, zl], j, 1, zl_id(dz))

    def t3(j):
        arrived(j, 1)
        total = zr2[j, 0]
        for i in range(1, NZL):
            total += zr2[j, i]
        factor = 1.0 if j < STREAMS else 1.0 / stretch
        zg[j, y] = (total * factor).astype(BF16).astype(F32)
        for dy in (1, 2, 3):
            send(zg.at[j, y], zg.at[j, y], j, 2, y_id(dy))

    def block(j, owner):
        z = zg[j].reshape(depth, rows).astype(BF16)
        return jnp.dot(
            z, a[:, pl.ds(pl.multiple_of(owner * group, group), group)],
            preferred_element_type=F32,
        )

    def pieces(j):
        return [(j * PARTS + h, slice(h * sub, (h + 1) * sub)) for h in range(PARTS)]

    def t4(j):
        arrived(j, 2)
        value = block(j, across["x"]).astype(BF16)
        for i, r in pieces(j):
            far[i, 0] = value[r, :half]
            far[i, 1] = value[r, half:]
            straight = i in STRAIGHT_SUMS
            send(far.at[i, 0], passed.at[i, 0], i, 3, across if straight else right)
            send(far.at[i, 1], passed.at[i, 1], i, 3, across if straight else left)

    def t9(j):
        value = block(j, right["x"])
        for i, r in pieces(j):
            if i in STRAIGHT_SUMS:
                far[i, 2] = value[r, :half].astype(BF16)
                send(far.at[i, 2], yr.at[i, 0, 0], i, 4, right)
            else:
                held[i, 0] = value[r, :half]
            alone[i, 0] = value[r, half:].astype(BF16)
            send(alone.at[i, 0], yr.at[i, 0, 1], i, 4, right)
        value = block(j, left["x"])
        for i, r in pieces(j):
            if i in STRAIGHT_SUMS:
                far[i, 3] = value[r, half:].astype(BF16)
                send(far.at[i, 3], yr.at[i, 1, 1], i, 4, left)
            else:
                held[i, 1] = value[r, half:]
            alone[i, 1] = value[r, :half].astype(BF16)
            send(alone.at[i, 1], yr.at[i, 1, 0], i, 4, left)
        value = block(j, x)
        for i, r in pieces(j):
            yown[i] = value[r]

    def t5(i):
        arrived(i, 3)
        for n, peer in enumerate((right, left)):
            far[i, 2 + n] = (held[i, n] + passed[i, n].astype(F32)).astype(BF16)
            send(far.at[i, 2 + n], yr.at[i, n, n], i, 4, peer)

    def t6(i):
        arrived(i, 4)
        if i in STRAIGHT_SUMS:
            arrived(i, 3)
        for n, cols in enumerate((low, high)):
            total = yown[i, :, cols] + yr[i, 0, n].astype(F32) + yr[i, 1, n].astype(F32)
            if i in STRAIGHT_SUMS:
                total += passed[i, n].astype(F32)
            hs[i, :, cols] = total.astype(BF16)
        send(hs.at[i], hr.at[i], i, 5, other)

    def t7(i):
        k, s, r = place_of(i)
        arrived(i, 5)
        total = (hs[i].astype(F32) + hr[i].astype(F32)) * stretch
        out[k, x, r, :] = total.astype(BF16)
        place = out.at[k, x, r]
        for peer in (right, left):
            send(place, place, i, 6, peer)
        if i in STRAIGHT_COPIES:
            send(place, place, i, 7, across)
        if k == 0 and whole(7, s):
            zpart[s] = term(s, x)

    def t8(i):
        k, s, r = place_of(i)
        arrived(i, 6)
        for source, cols, peer in ((left, low, right), (right, high, left)):
            if i in STRAIGHT_COPIES:
                break
            place = out.at[k, source["x"], r, cols]
            send(place, place, i, 7, peer)
        if k == 0 and whole(8, s):
            zpart[s] += term(s, right["x"]) + term(s, left["x"])

    for b in range(LOADS):
        for copy in loads[b]:
            copy.wait()
        product = jnp.dot(a[:, columns(b)], p[columns(b), :], preferred_element_type=F32)
        if b == 0:
            z1[...] = product
        else:
            z1[...] += product
    first = z1[...].T
    pl.semaphore_wait(barrier, len(peers))

    def t0(j):
        z_send(j, first[j * depth : (j + 1) * depth])

    def t10(q):
        cols = pl.ds(q * group, group)
        at[cols, :] = a[:, cols].T

    tasks = (t0, t1, t2, t3, t4, t5, t6, t7, t8, t9, t10)
    for task in PLAN:
        kind, j = divmod(task, 100)
        tasks[kind](j)
    for j, stage in sent:
        if (j, stage) not in got:
            arrived(j, stage)
    for j, stage in sent:
        done(j, stage).wait_send()


def turn(blocks, out, turned, sems):
    group = blocks.shape[3]
    copies = []
    for k in range(ITERS):
        for b in range(NX):
            rows = pl.ds(b * group, group)
            turned[k, rows, :] = blocks[k, b].T
            copy = pltpu.make_async_copy(turned.at[k, rows], out.at[k, rows], sems.at[k, b])
            copy.start()
            copies.append(copy)
    for copy in copies:
        copy.wait()


def body(matrix, probes):
    rows, width = matrix.shape
    probe = probes.shape[1]
    m_total = rows * SIZES[0] * SIZES[1]
    n_total = width * SIZES[2] * SIZES[3] * SIZES[4]
    group, depth = width // NX, probe // STREAMS
    part, half, count = depth // NY, group // 2, ITERS * STREAMS
    sub, pieces = depth // PARTS, ITERS * STREAMS * PARTS
    blocks = pl.pallas_call(
        functools.partial(kernel, math.sqrt(n_total / m_total)),
        out_shape=jax.ShapeDtypeStruct((ITERS, NX, probe, group), BF16),
        in_specs=[pl.BlockSpec(memory_space=pltpu.HBM)] * 2,
        out_specs=pl.BlockSpec(memory_space=pltpu.VMEM),
        scratch_shapes=[
            pltpu.VMEM((rows, width), BF16),
            pltpu.VMEM((width, rows), BF16),
            pltpu.VMEM((width, probe), BF16),
            pltpu.VMEM((rows, probe), F32),
            pltpu.VMEM((STREAMS, depth, rows), F32),
            pltpu.VMEM((count, NY, part, rows), F32),
            pltpu.VMEM((count, NY * NC, part, rows), F32),
            pltpu.VMEM((count, part, rows), F32),
            pltpu.VMEM((count, NZL, part, rows), F32),
            pltpu.VMEM((count, NY, part, rows), F32),
            pltpu.VMEM((pieces, 4, sub, half), BF16),
            pltpu.VMEM((pieces, 2, sub, half), BF16),
            pltpu.VMEM((pieces, 2, sub, half), F32),
            pltpu.VMEM((pieces, sub, group), F32),
            pltpu.VMEM((pieces, 2, sub, half), BF16),
            pltpu.VMEM((pieces, 2, 2, sub, half), BF16),
            pltpu.VMEM((pieces, sub, group), BF16),
            pltpu.VMEM((pieces, sub, group), BF16),
            pltpu.SemaphoreType.DMA((2, LOADS)),
            pltpu.SemaphoreType.DMA((count, 3)),
            pltpu.SemaphoreType.DMA((count, 3)),
            pltpu.SemaphoreType.DMA((pieces, 5)),
            pltpu.SemaphoreType.DMA((pieces, 5)),
        ],
        compiler_params=pltpu.CompilerParams(
            collective_id=0, has_side_effects=True, vmem_limit_bytes=44 * 1024 * 1024
        ),
    )(*(pltpu.with_memory_space_constraint(v, pltpu.HBM) for v in (matrix, probes)))
    return pl.pallas_call(
        turn,
        out_shape=jax.ShapeDtypeStruct((ITERS, width, probe), BF16),
        in_specs=[pl.BlockSpec(memory_space=pltpu.VMEM)],
        out_specs=pl.BlockSpec(memory_space=pl.ANY),
        scratch_shapes=[
            pltpu.VMEM((ITERS, width, probe), BF16),
            pltpu.SemaphoreType.DMA((ITERS, NX)),
        ],
        compiler_params=pltpu.CompilerParams(vmem_limit_bytes=24 * 1024 * 1024),
    )(blocks)


def solution(mesh):
    torus = Mesh(mesh.devices.reshape(SIZES), AXES)
    col = ("zl", "y", "core")
    return jax.shard_map(
        body, mesh=torus, in_specs=(P(("zh", "x"), col), P(col, None)),
        out_specs=P(None, col, None), check_vma=False,
    )
```

```python
import functools
import math

import jax
import jax.numpy as jnp
from jax import lax
from jax.experimental import pallas as pl
from jax.experimental.pallas import tpu as pltpu
from jax.sharding import Mesh
from jax.sharding import PartitionSpec as P

AXES = ("zh", "x", "zl", "y", "core")
SIZES = (2, 4, 4, 4, 2)
NX, NZL, NY, NC = 4, 4, 4, 2
ITERS = 2
STREAMS = 4
PARTS = 2
STRAIGHT_SUMS = (0, 1)
STRAIGHT_COPIES = (14, 15)
LOADS = 8
PLAN = (
    1, 0, 3, 2, 201, 200, 202, 301, 203, 300, 401, 303, 302, 400, 900, 402, 1000, 901, 1003, 502, 600, 403, 503,
    903, 1001, 601, 902, 504, 602, 603, 505, 700, 1002, 506, 701, 507, 604, 605, 702, 800, 801, 703, 607, 704, 606,
    802, 104, 803, 705, 707, 804, 105, 204, 706, 805, 807, 304, 205, 806, 106, 404, 305, 107, 904, 206, 508, 405,
    509, 207, 306, 905, 510, 511, 608, 307, 609, 406, 906, 407, 611, 512, 907, 610, 513, 514, 708, 612, 709, 711,
    614, 613, 515, 710, 808, 809, 811, 712, 615, 810, 714, 713, 812, 715, 813,
)
F32, BF16 = jnp.float32, jnp.bfloat16
MESH_ID = pl.DeviceIdType.MESH


def kernel(
    stretch,
    a_hbm, p_hbm, out,
    a, at, p, z1, zpart, zsend, zr1, zs2, zr2, zg, far, alone, held, yown, passed, yr, hs, hr,
    load_sem, z_send_sem, z_recv_sem, y_send_sem, y_recv_sem,
):
    rows, width = a.shape
    group = width // NX
    half = group // 2
    depth = out.shape[2] // STREAMS
    part = depth // NY
    sub = depth // PARTS
    step = width // LOADS
    x, zl, y, core = (lax.axis_index(n) for n in ("x", "zl", "y", "core"))
    zh = lax.axis_index("zh")
    me = y * NC + core

    def columns(b):
        return pl.ds(b * step, step)

    loads = []
    for b in range(LOADS):
        pair = (
            pltpu.make_async_copy(a_hbm.at[:, columns(b)], a.at[:, columns(b)], load_sem.at[0, b]),
            pltpu.make_async_copy(p_hbm.at[columns(b)], p.at[columns(b)], load_sem.at[1, b]),
        )
        for copy in pair:
            copy.start()
        loads.append(pair)

    near = [(dy, dc) for dy in range(NY) for dc in range(NC) if dy or dc]

    def near_id(dy, dc):
        return {"y": lax.rem(y + dy, NY), "core": lax.rem(core + dc, NC)}

    def x_id(dx):
        return {"x": lax.rem(x + dx, NX)}

    def zl_id(dz):
        return {"zl": lax.rem(zl + dz, NZL)}

    def y_id(dy):
        return {"y": lax.rem(y + dy, NY)}

    other = {"zh": 1 - zh}
    right, left, across = x_id(1), x_id(3), x_id(2)

    barrier = pltpu.get_barrier_semaphore()
    peers = [near_id(*d) for d in near] + [zl_id(d) for d in (1, 2, 3)]
    peers += [x_id(d) for d in (1, 2, 3)] + [other]
    for peer in peers:
        pl.semaphore_signal(barrier, inc=1, device_id=peer, device_id_type=MESH_ID)

    sent, got = {}, set()
    low, high = pl.ds(0, half), pl.ds(half, half)

    def sems(j, stage):
        if stage < 3:
            return {"send_sem": z_send_sem.at[j, stage], "recv_sem": z_recv_sem.at[j, stage]}
        return {"send_sem": y_send_sem.at[j, stage - 3], "recv_sem": y_recv_sem.at[j, stage - 3]}

    def send(src, dst, j, stage, peer):
        sent[j, stage] = 1
        pltpu.make_async_remote_copy(
            src_ref=src, dst_ref=dst, device_id=peer, device_id_type=MESH_ID, **sems(j, stage)
        ).start()

    def z_done(ref, j, stage):
        return pltpu.make_async_remote_copy(
            src_ref=ref, dst_ref=ref, device_id=other, device_id_type=MESH_ID, **sems(j, stage)
        )

    def done(j, stage):
        r = pl.ds(0, sub)
        ref = (
            lambda: passed.at[j], lambda: yr.at[j], lambda: hr.at[j],
            lambda: out.at[0, pl.ds(0, 2), r], lambda: out.at[0, 0, r],
        )[stage - 3]()
        return z_done(ref, j, stage)

    def arrived(j, stage):
        got.add((j, stage))
        done(j, stage).wait_recv()

    def stream_rows(s):
        return pl.ds(s * depth, depth)

    def place_of(i):
        j, h = divmod(i, PARTS)
        k, s = divmod(j, STREAMS)
        return k, s, pl.ds(s * depth + h * sub, sub)

    counts = {}

    def whole(kind, s):
        counts[kind, s] = counts.get((kind, s), 0) + 1
        return counts[kind, s] == PARTS

    def z_send(j, value):
        zsend[j] = value.reshape(NY, part, rows)
        for dy in (1, 2, 3):
            to = lax.rem(y + dy, NY)
            send(zsend.at[j, to], zr1.at[j, me], j, 0, {"y": to, "core": 1})

        @pl.when(core == 0)
        def _():
            send(zsend.at[j, y], zr1.at[j, me], j, 0, {"core": 1})

        @pl.when(core == 1)
        def _():
            zr1[j, me] = zsend[j, y]

    def term(s, owner):
        return jnp.dot(
            out[0, owner, stream_rows(s), :], at[pl.ds(pl.multiple_of(owner * group, group), group), :],
            preferred_element_type=F32,
        )

    def t1(j):
        s = j - STREAMS

        for h in range(PARTS):
            arrived(s * PARTS + h, 7)
        z_send(j, zpart[s] + term(s, across["x"]))

    def t2(j):
        @pl.when(core == 1)
        def _():
            z_done(zr1.at[j, pl.ds(0, NY * NC - 1)], j, 0).wait_recv()
            total = zr1[j, 0]
            for i in range(1, NY * NC):
                total += zr1[j, i]
            zs2[j] = total
            zr2[j, zl] = total
            for dz in (1, 2, 3):
                send(zs2.at[j], zr2.at[j, zl], j, 1, zl_id(dz))

    def t3(j):
        @pl.when(core == 1)
        def _():
            z_done(zr2.at[j, pl.ds(0, NZL - 1)], j, 1).wait_recv()
            total = zr2[j, 0]
            for i in range(1, NZL):
                total += zr2[j, i]
            factor = 1.0 if j < STREAMS else 1.0 / stretch
            zg[j, y] = (total * factor).astype(BF16).astype(F32)
            for dy in (1, 2, 3):
                for to in (0, 1):
                    send(zg.at[j, y], zg.at[j, y], j, 2, {**y_id(dy), "core": to})
            send(zg.at[j, y], zg.at[j, y], j, 2, {"core": 0})

    def z_ready(j):
        @pl.when(core == 0)
        def _():
            z_done(zg.at[j], j, 2).wait_recv()

        @pl.when(core == 1)
        def _():
            z_done(zg.at[j, pl.ds(0, NY - 1)], j, 2).wait_recv()

    def z_sent(j):
        @pl.when(core == 0)
        def _():
            z_done(zr1.at[j, pl.ds(0, NY)], j, 0).wait_send()

        @pl.when(core == 1)
        def _():
            z_done(zr1.at[j, pl.ds(0, NY - 1)], j, 0).wait_send()
            z_done(zr2.at[j, pl.ds(0, NZL - 1)], j, 1).wait_send()
            z_done(zr1.at[j, pl.ds(0, NY * NC - 1)], j, 2).wait_send()

    def block(j, owner):
        z = zg[j].reshape(depth, rows).astype(BF16)
        return jnp.dot(
            z, a[:, pl.ds(pl.multiple_of(owner * group, group), group)],
            preferred_element_type=F32,
        )

    def pieces(j):
        return [(j * PARTS + h, slice(h * sub, (h + 1) * sub)) for h in range(PARTS)]

    def t4(j):
        z_ready(j)
        value = block(j, across["x"]).astype(BF16)
        for i, r in pieces(j):
            far[i, 0] = value[r, :half]
            far[i, 1] = value[r, half:]
            straight = i in STRAIGHT_SUMS
            send(far.at[i, 0], passed.at[i, 0], i, 3, across if straight else right)
            send(far.at[i, 1], passed.at[i, 1], i, 3, across if straight else left)

    def t9(j):
        value = block(j, right["x"])
        for i, r in pieces(j):
            if i in STRAIGHT_SUMS:
                far[i, 2] = value[r, :half].astype(BF16)
                send(far.at[i, 2], yr.at[i, 0, 0], i, 4, right)
            else:
                held[i, 0] = value[r, :half]
            alone[i, 0] = value[r, half:].astype(BF16)
            send(alone.at[i, 0], yr.at[i, 0, 1], i, 4, right)
        value = block(j, left["x"])
        for i, r in pieces(j):
            if i in STRAIGHT_SUMS:
                far[i, 3] = value[r, half:].astype(BF16)
                send(far.at[i, 3], yr.at[i, 1, 1], i, 4, left)
            else:
                held[i, 1] = value[r, half:]
            alone[i, 1] = value[r, :half].astype(BF16)
            send(alone.at[i, 1], yr.at[i, 1, 0], i, 4, left)
        value = block(j, x)
        for i, r in pieces(j):
            yown[i] = value[r]

    def t5(i):
        arrived(i, 3)
        for n, peer in enumerate((right, left)):
            far[i, 2 + n] = (held[i, n] + passed[i, n].astype(F32)).astype(BF16)
            send(far.at[i, 2 + n], yr.at[i, n, n], i, 4, peer)

    def t6(i):
        arrived(i, 4)
        if i in STRAIGHT_SUMS:
            arrived(i, 3)
        for n, cols in enumerate((low, high)):
            total = yown[i, :, cols] + yr[i, 0, n].astype(F32) + yr[i, 1, n].astype(F32)
            if i in STRAIGHT_SUMS:
                total += passed[i, n].astype(F32)
            hs[i, :, cols] = total.astype(BF16)
        send(hs.at[i], hr.at[i], i, 5, other)

    def t7(i):
        k, s, r = place_of(i)
        arrived(i, 5)
        total = (hs[i].astype(F32) + hr[i].astype(F32)) * stretch
        out[k, x, r, :] = total.astype(BF16)
        place = out.at[k, x, r]
        for peer in (right, left):
            send(place, place, i, 6, peer)
        if i in STRAIGHT_COPIES:
            send(place, place, i, 7, across)
        if k == 0 and whole(7, s):
            zpart[s] = term(s, x)

    def t8(i):
        k, s, r = place_of(i)
        arrived(i, 6)
        for source, cols, peer in ((left, low, right), (right, high, left)):
            if i in STRAIGHT_COPIES:
                break
            place = out.at[k, source["x"], r, cols]
            send(place, place, i, 7, peer)
        if k == 0 and whole(8, s):
            zpart[s] += term(s, right["x"]) + term(s, left["x"])

    for b in range(LOADS):
        for copy in loads[b]:
            copy.wait()
        product = jnp.dot(a[:, columns(b)], p[columns(b), :], preferred_element_type=F32)
        if b == 0:
            z1[...] = product
        else:
            z1[...] += product
    first = z1[...].T
    pl.semaphore_wait(barrier, len(peers))

    def t0(j):
        z_send(j, first[j * depth : (j + 1) * depth])

    def t10(q):
        cols = pl.ds(q * group, group)
        at[cols, :] = a[:, cols].T

    tasks = (t0, t1, t2, t3, t4, t5, t6, t7, t8, t9, t10)
    for task in PLAN:
        kind, j = divmod(task, 100)
        tasks[kind](j)
    for j, stage in sent:
        if stage >= 3 and (j, stage) not in got:
            arrived(j, stage)
    for j in range(ITERS * STREAMS):
        z_sent(j)
    for j, stage in sent:
        if stage >= 3:
            done(j, stage).wait_send()


def turn(blocks, out, turned, sems):
    group = blocks.shape[3]
    copies = []
    for k in range(ITERS):
        for b in range(NX):
            rows = pl.ds(b * group, group)
            turned[k, rows, :] = blocks[k, b].T
            copy = pltpu.make_async_copy(turned.at[k, rows], out.at[k, rows], sems.at[k, b])
            copy.start()
            copies.append(copy)
    for copy in copies:
        copy.wait()


def body(matrix, probes):
    rows, width = matrix.shape
    probe = probes.shape[1]
    m_total = rows * SIZES[0] * SIZES[1]
    n_total = width * SIZES[2] * SIZES[3] * SIZES[4]
    group, depth = width // NX, probe // STREAMS
    part, half, count = depth // NY, group // 2, ITERS * STREAMS
    sub, pieces = depth // PARTS, ITERS * STREAMS * PARTS
    blocks = pl.pallas_call(
        functools.partial(kernel, math.sqrt(n_total / m_total)),
        out_shape=jax.ShapeDtypeStruct((ITERS, NX, probe, group), BF16),
        in_specs=[pl.BlockSpec(memory_space=pltpu.HBM)] * 2,
        out_specs=pl.BlockSpec(memory_space=pltpu.VMEM),
        scratch_shapes=[
            pltpu.VMEM((rows, width), BF16),
            pltpu.VMEM((width, rows), BF16),
            pltpu.VMEM((width, probe), BF16),
            pltpu.VMEM((rows, probe), F32),
            pltpu.VMEM((STREAMS, depth, rows), F32),
            pltpu.VMEM((count, NY, part, rows), F32),
            pltpu.VMEM((count, NY * NC, part, rows), F32),
            pltpu.VMEM((count, part, rows), F32),
            pltpu.VMEM((count, NZL, part, rows), F32),
            pltpu.VMEM((count, NY, part, rows), F32),
            pltpu.VMEM((pieces, 4, sub, half), BF16),
            pltpu.VMEM((pieces, 2, sub, half), BF16),
            pltpu.VMEM((pieces, 2, sub, half), F32),
            pltpu.VMEM((pieces, sub, group), F32),
            pltpu.VMEM((pieces, 2, sub, half), BF16),
            pltpu.VMEM((pieces, 2, 2, sub, half), BF16),
            pltpu.VMEM((pieces, sub, group), BF16),
            pltpu.VMEM((pieces, sub, group), BF16),
            pltpu.SemaphoreType.DMA((2, LOADS)),
            pltpu.SemaphoreType.DMA((count, 3)),
            pltpu.SemaphoreType.DMA((count, 3)),
            pltpu.SemaphoreType.DMA((pieces, 5)),
            pltpu.SemaphoreType.DMA((pieces, 5)),
        ],
        compiler_params=pltpu.CompilerParams(
            collective_id=0, has_side_effects=True, vmem_limit_bytes=44 * 1024 * 1024
        ),
    )(*(pltpu.with_memory_space_constraint(v, pltpu.HBM) for v in (matrix, probes)))
    return pl.pallas_call(
        turn,
        out_shape=jax.ShapeDtypeStruct((ITERS, width, probe), BF16),
        in_specs=[pl.BlockSpec(memory_space=pltpu.VMEM)],
        out_specs=pl.BlockSpec(memory_space=pl.ANY),
        scratch_shapes=[
            pltpu.VMEM((ITERS, width, probe), BF16),
            pltpu.SemaphoreType.DMA((ITERS, NX)),
        ],
        compiler_params=pltpu.CompilerParams(vmem_limit_bytes=24 * 1024 * 1024),
    )(blocks)


def solution(mesh):
    torus = Mesh(mesh.devices.reshape(SIZES), AXES)
    col = ("zl", "y", "core")
    return jax.shard_map(
        body, mesh=torus, in_specs=(P(("zh", "x"), col), P(col, None)),
        out_specs=P(None, col, None), check_vma=False,
    )
```
